32 devices in a mesh: section: 4 (over y, x), vocab: 2 (over core), dp: 4 (over z).
Axes of the slice: x: 2, y: 2, z: 4, core: 2. Of those that a mesh axis runs over, the one named last changes fastest.
Arguments:
- entering: bfloat16 [8, 4, 32, 2048], P(None, 'dp', 'vocab'), may hold values from -6 to 6
- depths: int32 [8], replicated, may hold values from 1 to 4
- targets: int32 [8, 4, 32], P(None, 'dp'), may hold values from 0 to 64127
- norm_gain: float32 [4, 2048], P('section'), may hold values from 0.5 to 1.5
- w_gate: bfloat16 [4, 2048, 7168], P('section', 'dp', 'vocab'), may hold values from -0.125 to 0.125
- w_up: bfloat16 [4, 2048, 7168], P('section', 'dp', 'vocab'), may hold values from -0.125 to 0.125
- w_down: bfloat16 [4, 7168, 2048], P('section', 'vocab', 'dp'), may hold values from -0.0625 to 0.0625
- final_gain: float32 [2048], replicated, may hold values from 0.5 to 1.5
- head_weight: bfloat16 [2048, 64128], P(None, ('section', 'vocab')), may hold values from -32 to 32
Outputs:
- token_loss: float32 [8, 4, 32], P(None, 'dp')
- mean_loss: float32 [], replicated
The draws below stay inside these ranges and needn't reach their ends.
All inputs are finite; a program needn't handle non-finite values.
Results may differ from the reference program's by a relative error of at most 0.0055.
Values may be sent and summed in bfloat16 or wider, within the bound.
No kernel may reach another device: no remote copies, remote signals or barrier semaphores. Data moves between devices by JAX's collectives and lax.ppermute only.
A program may use at most 192 MiB of HBM per device.

```python
import math
import jax
import jax.numpy as jnp
import numpy as np
from jax import lax

D = 2048
FF = 7168
VOCAB = 64128
MICRO = 8
LAYERS = 4
POS = 32
REPLICAS = 4


def draw_head_weight(key, part):
    key_base = jax.random.fold_in(key, 11)
    column_pos = jnp.arange(VOCAB, dtype=jnp.float32)
    spread = 2.7 + 0.5 * column_pos / VOCAB
    result = jax.random.normal(key_base, (D, VOCAB), jnp.float32) * spread[None, :] / math.sqrt(D)
    result = jnp.clip(result, -32.0, 32.0)
    return result.astype(jnp.bfloat16)


def place_ends(values, rng, smallest, top_value):
    longest = values.shape.index(max(values.shape))
    spots = []
    for shift in (0, 1):
        where = [jax.random.randint(jax.random.fold_in(rng, axis), (), 0, length) for axis, length in enumerate(values.shape)]
        where[longest] = (where[longest] + shift) % values.shape[longest]
        spots.append(tuple(where))
    return values.at[spots[0]].set(smallest).at[spots[1]].set(top_value)


def shard_levels(stream_key, extent, cuts, least, top_value):
    def one(dim, parts):
        steps = jax.random.uniform(jax.random.fold_in(jax.random.fold_in(stream_key, 6), dim), (parts,), jnp.float32, least / len(cuts), top_value / len(cuts))
        return jnp.repeat(jnp.exp(steps), extent[dim] // parts).reshape((-1,) + (1,) * (len(extent) - dim - 1))

    level = one(*cuts[0])
    for cut in cuts[1:]:
        level = level * one(*cut)
    return level


def rank_bounds(amount, slope):
    weights = [(1 << 20) // math.isqrt(standing ** slope) + 1 for standing in range(1, amount + 1)]
    deviation = 1 + sum(weights) // (1 << 30)
    return np.cumsum(np.array([max(1, weight // deviation) for weight in weights]))


def ranked(own_key, dims, count, lean):
    grid = rank_bounds(count, lean)
    ticket = jax.random.randint(jax.random.fold_in(own_key, 1), dims, 0, int(grid[count - 1]))
    standing = jnp.searchsorted(jnp.asarray(grid, jnp.int32), ticket, side="right")
    return jax.random.permutation(jax.random.fold_in(own_key, 2), count)[standing].astype(jnp.int32)


def scatter_about(own_key, shape, deviation, most, shards=(), held_as=jnp.bfloat16):
    level = shard_levels(own_key, shape, shards, -0.22, 0.18) if shards else 1.0
    values = jax.random.normal(own_key, shape, jnp.float32) * deviation * level
    return jnp.minimum(jnp.maximum(values, -most), most).astype(held_as)


def setup_inputs(seed: int = 0) -> dict:
    key_of = jax.random.split(jax.random.key(seed), 10)
    entering = scatter_about(key_of[0], (MICRO, REPLICAS, POS, D), 1.0, 6.0, ((1, 4), (2, 2)))
    depths = place_ends(jax.random.randint(key_of[1], (MICRO,), 1, LAYERS + 1), jax.random.fold_in(key_of[1], 1), 1, LAYERS).astype(jnp.int32)
    targets = place_ends(ranked(key_of[2], (MICRO, REPLICAS, POS), VOCAB, 2), jax.random.fold_in(key_of[2], 3), 0, VOCAB - 1).astype(jnp.int32)
    norm_gain = jnp.clip(1.0 + 0.1 * jax.random.normal(key_of[3], (LAYERS, D), jnp.float32), 0.5, 1.5)
    w_gate = scatter_about(key_of[4], (LAYERS, D, FF), D ** -0.5, 0.125, ((0, 4), (1, 4), (2, 2)))
    w_up = scatter_about(key_of[5], (LAYERS, D, FF), D ** -0.5, 0.125, ((0, 4), (1, 4), (2, 2)))
    w_down = scatter_about(key_of[6], (LAYERS, FF, D), FF ** -0.5, 0.0625, ((0, 4), (1, 2), (2, 4)))
    final_gain = jnp.clip(1.0 + 0.1 * jax.random.normal(key_of[7], (D,), jnp.float32), 0.5, 1.5)
    head_weight = draw_head_weight(jax.random.fold_in(key_of[9], 71), 0)
    return dict(entering=entering, depths=depths, targets=targets, norm_gain=norm_gain, w_gate=w_gate, w_up=w_up, w_down=w_down, final_gain=final_gain, head_weight=head_weight)


EPS = 1e-05

def rms_scaled(values, gain):
    widened = values.astype(jnp.float32)
    return widened * lax.rsqrt(lax.optimization_barrier(jnp.mean(widened * widened, axis=-1, keepdims=True)) + EPS) * gain

def reference(entering, depths, targets, norm_gain, w_gate, w_up, w_down, final_gain, head_weight):
    micro_count = entering.shape[0]
    width = entering.shape[3]
    current = entering.reshape(micro_count, -1, width)
    labels = targets.reshape(micro_count, -1)

    def run_layer(carried, layer_args):
        gain, gate_matrix, up_matrix, down_matrix, layer_index = layer_args
        normed = rms_scaled(carried, gain).astype(jnp.bfloat16).reshape(-1, width)
        gate_part = jnp.dot(normed, gate_matrix, preferred_element_type=jnp.float32)
        up_part = jnp.dot(normed, up_matrix, preferred_element_type=jnp.float32)
        hidden = (jax.nn.silu(gate_part) * up_part).astype(jnp.bfloat16)
        branch = jnp.dot(hidden, down_matrix, preferred_element_type=jnp.float32).reshape(carried.shape)
        moved = (carried.astype(jnp.float32) + branch).astype(jnp.bfloat16)
        active = (layer_index < depths)[:, None, None]
        return (jnp.where(active, moved, carried), None)
    layer_ids = jnp.arange(LAYERS, dtype=jnp.int32)
    current, unused = lax.scan(run_layer, current, (norm_gain, w_gate, w_up, w_down, layer_ids))
    finals = rms_scaled(current, final_gain).astype(jnp.bfloat16)

    def one_batch(batch_args):
        rows_now, labels_now = batch_args
        logits = jnp.dot(rows_now, head_weight, preferred_element_type=jnp.float32)
        peak = lax.optimization_barrier(jnp.max(logits, axis=-1, keepdims=True))
        spread_sum = jnp.log(lax.optimization_barrier(jnp.sum(jnp.exp(logits - peak), axis=-1))) + peak[:, 0]
        picked = jnp.take_along_axis(logits, labels_now[:, None].astype(jnp.int32), axis=1)[:, 0]
        return spread_sum - picked
    losses = lax.map(one_batch, (finals, labels))
    token_loss = losses.reshape(targets.shape)
    return (token_loss, jnp.mean(losses))
```

```python
import jax
import jax.numpy as jnp
from jax import lax
from jax.sharding import PartitionSpec as P

EPS = 1e-05
MESH_AXES = ("section", "vocab", "dp")


def rms_scaled(values, gain):
    widened = values.astype(jnp.float32)
    return widened * lax.rsqrt(jnp.mean(widened * widened, axis=-1, keepdims=True) + EPS) * gain


def combine_rows(first_stats, second_stats):
    peak_one, total_one, picked_one = first_stats
    peak_two, total_two, picked_two = second_stats
    peak_new = jnp.maximum(peak_one, peak_two)
    total_new = total_one * jnp.exp(peak_one - peak_new) + total_two * jnp.exp(peak_two - peak_new)
    return (peak_new, total_new, picked_one + picked_two)


def swapped(block, axis, mask, targets=None):
    size = lax.axis_size(axis)
    pairs = [(i, i ^ mask) for i in range(size) if targets is None or (i ^ mask) in targets]
    return lax.ppermute(block, axis, pairs)


def chosen(options, index):
    result = options[0]
    for k in range(1, len(options)):
        result = jnp.where(index == k, options[k], result)
    return result


def absolute(values, index, axis, size):
    bit = 1
    while bit < size:
        order = jnp.array([i ^ bit for i in range(size)])
        flipped = jnp.concatenate(
            [lax.index_in_dim(values, i ^ bit, axis, True) for i in range(size)], axis
        )
        del order
        values = jnp.where((index & bit) != 0, flipped, values)
        bit *= 2
    return values


def by_planes(entering, depths, targets, norm_gain, w_gate, w_up, w_down, final_gain, head_weight):
    sections = lax.axis_size("section")
    cores = lax.axis_size("vocab")
    my_column = lax.axis_index("section")
    my_core = lax.axis_index("vocab")
    my_plane = lax.axis_index("dp")
    micro_count, _, rows_each, width = entering.shape
    layers = sections
    first_plane = sections // 2 - 1
    plane_of = [(first_plane + layer) % sections for layer in range(layers)]
    my_layer = (my_plane - first_plane) % sections

    def linear(section, core, plane):
        return (section * cores + core) * sections + plane

    micro_ids = jnp.arange(micro_count, dtype=jnp.int32)
    deeper = (depths[None, :] > depths[:, None]) | (
        (depths[None, :] == depths[:, None]) & (micro_ids[None, :] < micro_ids[:, None])
    )
    rank = jnp.sum(deeper.astype(jnp.int32), axis=1)
    hot = rank[None, :] == micro_ids[:, None]
    order = jnp.sum(jnp.where(hot, micro_ids[None, :], 0), axis=1)
    sorted_depths = jnp.sum(jnp.where(hot, depths[None, :], 0), axis=1)
    active_counts = [jnp.sum((depths > layer).astype(jnp.int32)) for layer in range(layers + 1)]

    hidden_each = w_gate.shape[2] // sections
    feature_each = w_gate.shape[1]

    def column_block(matrix, column):
        if matrix is w_down:
            return lax.dynamic_slice_in_dim(matrix[0], column * hidden_each, hidden_each, 0)
        return lax.dynamic_slice_in_dim(matrix[0], column * hidden_each, hidden_each, 1)

    def across(matrix):
        return [
            column_block(matrix, my_column)
            if mask == 0
            else swapped(column_block(matrix, my_column ^ mask), "section", mask)
            for mask in range(sections)
        ]

    def layer_at(plane):
        return (plane - first_plane) % sections

    early_planes = plane_of[:2]
    late_planes = plane_of[2:]

    def towards(held, planes, axis):
        mine = chosen(held, my_layer ^ my_column)
        shape = list(mine.shape)
        shape[axis] = shape[axis] * sections
        whole = jnp.zeros(shape, mine.dtype)
        whole = lax.dynamic_update_slice_in_dim(whole, mine, my_plane * feature_each, axis)
        for mask in (2, 3, 1):
            block = chosen(held, layer_at(my_plane ^ mask) ^ my_column)
            arrived = swapped(block, "dp", mask, planes)
            whole = lax.dynamic_update_slice_in_dim(
                whole, arrived, (my_plane ^ mask) * feature_each, axis
            )
        return whole

    gates, ups, downs = across(w_gate), across(w_up), across(w_down)
    early = (towards(gates, early_planes, 0), towards(ups, early_planes, 0), towards(downs, early_planes, 1))
    late = (towards(gates, late_planes, 0), towards(ups, late_planes, 0), towards(downs, late_planes, 1))

    gains = [norm_gain] + [swapped(norm_gain, "section", mask) for mask in range(1, sections)]
    my_gain = chosen(gains, my_layer ^ my_column)
    labels_by = [targets[:, 0]] + [swapped(targets[:, 0], "dp", mask) for mask in range(1, sections)]
    labels_all = absolute(jnp.stack(labels_by), my_plane, 0, sections)

    def spread_rows(rows):
        own = jnp.concatenate(
            [rows] + [swapped(rows, "section", mask) for mask in range(1, sections)], 0
        )
        return jnp.concatenate([own, swapped(own, "vocab", 1)], 0)

    def collected(partial):
        half = partial.shape[0] // cores
        own = partial[:half] + swapped(partial[half:], "vocab", 1)
        each = half // sections
        total = own[:each]
        for mask in range(1, sections):
            sent = own[mask * each : (mask + 1) * each].astype(jnp.bfloat16)
            total = total + swapped(sent, "section", mask).astype(jnp.float32)
        return total

    def run_layer(layer, state, weights, count):
        gate, up, down = weights
        current = state[:count].reshape(count * rows_each, width)
        rows = spread_rows(rms_scaled(current, my_gain).astype(jnp.bfloat16))
        gate_part = jnp.dot(rows, gate, preferred_element_type=jnp.float32)
        up_part = jnp.dot(rows, up, preferred_element_type=jnp.float32)
        hidden = (jax.nn.silu(gate_part) * up_part).astype(jnp.bfloat16)
        branch = collected(jnp.dot(hidden, down, preferred_element_type=jnp.float32))
        moved = (current.astype(jnp.float32) + branch).astype(jnp.bfloat16)
        keep = (sorted_depths[:count] > layer)[:, None, None]
        moved = jnp.where(keep, moved.reshape(count, rows_each, width), state[:count])
        if count < micro_count:
            moved = jnp.concatenate([moved, state[count:]], 0)
        return moved

    def handed_on(state, layer, count):
        pairs = [
            (linear(s, c, plane_of[layer - 1]), linear(s, c, plane_of[layer]))
            for s in range(sections)
            for c in range(cores)
        ]
        arrived = lax.ppermute(state[:count], MESH_AXES, pairs)
        if count < micro_count:
            arrived = jnp.concatenate([arrived, state[count:]], 0)
        return jnp.where(my_plane == plane_of[layer], arrived, state)

    sorted_rows = jnp.concatenate(
        [lax.dynamic_slice_in_dim(entering[:, 0], order[i], 1, 0) for i in range(micro_count)], 0
    )
    pairs = [
        (linear(s, c, s), linear(s, c, plane_of[0])) for s in range(sections) for c in range(cores)
    ]
    state = lax.ppermute(sorted_rows, MESH_AXES, pairs)
    state = run_layer(0, state, early, micro_count)
    sizes = [n for n in range(2, micro_count + 1, 2)]
    for layer in range(1, layers):
        weights = early if layer < 2 else late

        def branch_of(count, layer=layer):
            return lambda state, weights: run_layer(
                layer, handed_on(state, layer, count), weights, count
            )

        which = jnp.clip((active_counts[layer] + 1) // 2 - 1, 0, len(sizes) - 1)
        state = lax.switch(which, [branch_of(n) for n in sizes], state, weights)

    exits_from = chosen(active_counts[1:], my_layer)
    exits_to = chosen(active_counts[:layers], my_layer)
    exit_count = exits_to - exits_from
    most = active_counts[0] - active_counts[1]
    for layer in range(1, layers):
        most = jnp.maximum(most, active_counts[layer] - active_counts[layer + 1])
    column_count = head_weight.shape[1]
    first_column = (my_column * cores + my_core) * column_count
    labels_sorted = jnp.concatenate(
        [lax.dynamic_slice_in_dim(labels_all, order[i], 1, 1) for i in range(micro_count)], 1
    )

    def head(count):
        def run(state, head_weight):
            def window(array, axis):
                padding = [(0, 0)] * array.ndim
                padding[axis] = (0, micro_count)
                return lax.dynamic_slice_in_dim(jnp.pad(array, padding), exits_from, count, axis)

            leaving = window(state, 0).reshape(count * rows_each, width)
            finals = rms_scaled(leaving, final_gain).astype(jnp.bfloat16)
            rows = spread_rows(finals)
            logits = jnp.dot(rows, head_weight, preferred_element_type=jnp.float32)
            labels = window(labels_sorted, 1).reshape(sections, count, cores, rows_each)
            labels = labels.transpose(2, 0, 1, 3)
            labels = absolute(absolute(labels, my_core, 0, cores), my_column, 1, sections)
            labels = labels.reshape(-1)
            columns = first_column + jnp.arange(column_count, dtype=jnp.int32)
            picked = jnp.sum(jnp.where(columns == labels[:, None], logits, 0.0), axis=-1)
            peak = jnp.max(logits, axis=-1)
            total = jnp.sum(jnp.exp(logits - peak[:, None]), axis=-1)
            stats = jnp.stack([peak, total, picked]).reshape(3, cores, sections, -1)
            stats = absolute(absolute(stats, my_core, 1, cores), my_column, 2, sections)
            every = lax.all_gather(stats, ("section", "vocab"))
            joined = (every[0, 0], every[0, 1], every[0, 2])
            for i in range(1, sections * cores):
                joined = combine_rows(joined, (every[i, 0], every[i, 1], every[i, 2]))
            losses = jnp.log(joined[1]) + joined[0] - joined[2]
            losses = losses.reshape(cores, sections, count, rows_each).transpose(2, 1, 0, 3)
            losses = losses.reshape(count, sections, cores * rows_each)
            inside = jnp.arange(count) < exit_count
            losses = jnp.where(inside[:, None, None], losses, 0.0)
            table = jnp.zeros((2 * micro_count,) + losses.shape[1:], jnp.float32)
            table = lax.dynamic_update_slice_in_dim(table, losses, exits_from, 0)[:micro_count]
            return table

        return run

    which = jnp.clip((most + 1) // 2 - 1, 0, len(sizes) - 1)
    table = lax.switch(which, [head(n) for n in sizes], state, head_weight)
    for mask in (1, 2):
        table = table + swapped(table, "dp", mask)
    mean_loss = jnp.sum(table) / float(table.size)
    token_loss = jnp.sum(jnp.where(hot[:, :, None, None], table[:, None], 0.0), axis=0)
    token_loss = lax.dynamic_slice_in_dim(token_loss, my_plane, 1, 1)
    return (token_loss, mean_loss)


def passed_along(block, axis, distance):
    devices = range(lax.axis_size(axis))
    route = [(i - distance, i) for i in devices if i - distance in devices]
    return lax.ppermute(block, axis, route)


def spread(value, axis, source):
    kept = jnp.where(lax.axis_index(axis) == source, value, 0).astype(value.dtype)
    return lax.psum(kept, axis)


def joined(part, axis, combine):
    gathered = jax.tree.map(lambda a: lax.all_gather(a, axis), part)

    def take(source):
        return jax.tree.map(lambda a: lax.dynamic_index_in_dim(a, source, 0, False), gathered)

    return lax.fori_loop(
        1, lax.axis_size(axis), lambda source, state: combine(state, take(source)), take(0)
    )


def by_sections(entering, depths, targets, norm_gain, w_gate, w_up, w_down, final_gain, head_weight):
    segment_count = lax.axis_size("section")
    my_segment = lax.axis_index("section")
    micro_count = entering.shape[0]
    row_count = entering.shape[2]
    width = entering.shape[3]
    per_segment = w_gate.shape[0]
    gate_full, up_full, down_full = (
        lax.all_gather(w_gate, "dp", axis=1, tiled=True),
        lax.all_gather(w_up, "dp", axis=1, tiled=True),
        lax.all_gather(w_down, "dp", axis=2, tiled=True),
    )
    local_rows = entering[:, 0]

    def apply_layer(layer_index, current):
        normed = rms_scaled(current, norm_gain[layer_index]).astype(jnp.bfloat16)
        block_rows = lax.all_gather(normed, "vocab", axis=0, tiled=True)
        gate_part = jnp.dot(block_rows, gate_full[layer_index], preferred_element_type=jnp.float32)
        up_part = jnp.dot(block_rows, up_full[layer_index], preferred_element_type=jnp.float32)
        hidden = (jax.nn.silu(gate_part) * up_part).astype(jnp.bfloat16)
        branch = lax.psum_scatter(
            jnp.dot(hidden, down_full[layer_index], preferred_element_type=jnp.float32),
            "vocab",
            scatter_dimension=0,
            tiled=True,
        )
        return (current.astype(jnp.float32) + branch).astype(jnp.bfloat16)

    inject_order = jnp.arange(micro_count, dtype=jnp.int32)

    def advance(step_index, carry):
        current, kept_rows = carry
        slot_index = step_index - my_segment
        is_valid = (slot_index >= 0) & (slot_index < micro_count)
        member = inject_order[jnp.clip(slot_index, 0, micro_count - 1)]
        depth_now = jnp.where(is_valid, depths[member], 0)
        fresh_rows = lax.dynamic_index_in_dim(local_rows, member, 0, keepdims=False)
        current = jnp.where(my_segment == 0, fresh_rows, current)
        updated = apply_layer(0, current)
        current = jnp.where(my_segment * per_segment + 0 < depth_now, updated, current)
        record = is_valid & (my_segment == segment_count - 1)
        record_value = current
        previous = lax.dynamic_index_in_dim(kept_rows, member, 0, keepdims=False)
        kept_rows = lax.dynamic_update_index_in_dim(
            kept_rows, jnp.where(record, record_value, previous), member, 0
        )
        current = passed_along(current, "section", 1)
        return (current, kept_rows)

    start_rows = jnp.zeros((row_count, width), jnp.bfloat16)
    start_kept = jnp.zeros((micro_count, row_count, width), jnp.bfloat16)
    current, kept_rows = lax.fori_loop(
        0, micro_count + segment_count - 1, advance, (start_rows, start_kept)
    )
    finals = rms_scaled(kept_rows, final_gain).astype(jnp.bfloat16)
    finals = spread(finals, "section", segment_count - 1)
    share_rows = lax.all_gather(finals, "vocab", axis=1, tiled=True)
    labels = targets[:, 0]
    column_count = head_weight.shape[1]
    first_column = (my_segment * lax.axis_size("vocab") + lax.axis_index("vocab")) * column_count
    logits = jnp.einsum("mpd,dc->mpc", share_rows, head_weight, preferred_element_type=jnp.float32)
    columns = first_column + jnp.arange(column_count, dtype=jnp.int32)
    picked = jnp.sum(jnp.where(columns == labels[:, :, None], logits, 0.0), axis=-1)
    local_peak = jnp.max(logits, axis=-1)
    local_total = jnp.sum(jnp.exp(logits - local_peak[:, :, None]), axis=-1)
    peak_all, totals, target_logit = joined(
        (local_peak, local_total, picked), ("section", "vocab"), combine_rows
    )
    losses = jnp.log(totals) + peak_all - target_logit
    share_sum = lax.psum(jnp.sum(losses), "dp")
    mean_loss = share_sum / float(micro_count * lax.axis_size("dp") * losses.shape[1])
    return (losses[:, None, :], mean_loss)


def solution(mesh):
    in_specs = (
        P(None, "dp", "vocab", None),
        P(),
        P(None, "dp", None),
        P("section", None),
        P("section", "dp", "vocab"),
        P("section", "dp", "vocab"),
        P("section", "vocab", "dp"),
        P(),
        P(None, ("section", "vocab")),
    )
    out_specs = (P(None, "dp", None), P())
    square = mesh.shape["section"] == mesh.shape["dp"] == 4 and mesh.shape["vocab"] == 2
    on_device = by_planes if square else by_sections
    return jax.shard_map(
        on_device, mesh=mesh, in_specs=in_specs, out_specs=out_specs, check_vma=False
    )
```

```python
import jax
import jax.numpy as jnp
from jax import lax
from jax.experimental import pallas as pl
from jax.experimental.pallas import tpu as pltpu
from jax.sharding import PartitionSpec as P


EPS = 1e-05
MESH_AXES = ("section", "vocab", "dp")


def rms_scaled(values, gain):
    widened = values.astype(jnp.float32)
    return widened * lax.rsqrt(jnp.mean(widened * widened, axis=-1, keepdims=True) + EPS) * gain


def combine_rows(first_stats, second_stats):
    peak_one, total_one, picked_one = first_stats
    peak_two, total_two, picked_two = second_stats
    peak_new = jnp.maximum(peak_one, peak_two)
    total_new = total_one * jnp.exp(peak_one - peak_new) + total_two * jnp.exp(peak_two - peak_new)
    return (peak_new, total_new, picked_one + picked_two)


def swapped(block, axis, mask, targets=None):
    size = lax.axis_size(axis)
    pairs = [(i, i ^ mask) for i in range(size) if targets is None or (i ^ mask) in targets]
    return lax.ppermute(block, axis, pairs)


def chosen(options, index):
    result = options[0]
    for k in range(1, len(options)):
        result = jnp.where(index == k, options[k], result)
    return result


def absolute(values, index, axis, size):
    bit = 1
    while bit < size:
        flipped = jnp.concatenate(
            [lax.index_in_dim(values, i ^ bit, axis, True) for i in range(size)], axis
        )
        values = jnp.where((index & bit) != 0, flipped, values)
        bit *= 2
    return values


def after(value, *others):
    return lax.optimization_barrier((value,) + others)[0]


def layer_body(plane, *refs, pieces, blocks, steps):
    rows, refs = refs[:pieces], refs[pieces:]
    gates, ups, downs = refs[:blocks], refs[blocks : 2 * blocks], refs[2 * blocks : 3 * blocks]
    refs = refs[3 * blocks :]
    kept, sent = refs[: pieces // 2], refs[pieces // 2 : pieces]
    gathered, total = refs[pieces:]
    each = rows[0].shape[0]
    features = gates[0].shape[0]
    step = pl.program_id(0)

    def place(mask):
        return pl.ds(pl.multiple_of((plane[0] ^ mask) * features, features), features)

    @pl.when(step == 0)
    def _():
        for i in range(pieces):
            for mask in range(blocks):
                gathered[pl.ds(i * each, each), mask * features : (mask + 1) * features] = rows[i][
                    :, place(mask)
                ]

    count = pieces * each
    tile = min(count, 256)

    def tile_products(index, carry):
        first = pl.multiple_of(index * tile, tile)

        def product(matrices):
            result = None
            for mask in range(blocks):
                here = gathered[pl.ds(first, tile), mask * features : (mask + 1) * features]
                part = jnp.dot(here, matrices[mask][...], preferred_element_type=jnp.float32)
                result = part if result is None else result + part
            return result

        gate_part = product(gates)
        up_part = product(ups)
        hidden = (gate_part / (1.0 + jnp.exp(-gate_part)) * up_part).astype(jnp.bfloat16)
        for mask in range(blocks):
            part = jnp.dot(hidden, downs[mask][...], preferred_element_type=jnp.float32)
            columns = slice(mask * features, (mask + 1) * features)

            @pl.when(step == 0)
            def _(part=part, columns=columns):
                total[pl.ds(first, tile), columns] = part

            @pl.when(step > 0)
            def _(part=part, columns=columns):
                total[pl.ds(first, tile), columns] += part

        return carry

    lax.fori_loop(0, count // tile, tile_products, 0)

    @pl.when(step == steps - 1)
    def _():
        for i in range(pieces):
            for mask in range(blocks):
                block = total[pl.ds(i * each, each), mask * features : (mask + 1) * features]
                if i < pieces // 2:
                    kept[i][:, place(mask)] = block
                else:
                    sent[i - pieces // 2][:, place(mask)] = block.astype(jnp.bfloat16)


def layer_products(rows, weights, plane):
    gates, ups, downs = weights
    pieces, blocks = len(rows), len(gates)
    each, width = rows[0].shape
    features, hidden = gates[0].shape
    steps = 2 if hidden % 256 == 0 else 1
    part = hidden // steps
    whole = pl.BlockSpec((each, width), lambda i, plane: (0, 0))
    results = pl.pallas_call(
        lambda *refs: layer_body(*refs, pieces=pieces, blocks=blocks, steps=steps),
        grid_spec=pltpu.PrefetchScalarGridSpec(
            num_scalar_prefetch=1,
            grid=(steps,),
            in_specs=[whole] * pieces
            + [pl.BlockSpec((features, part), lambda i, plane: (0, i))] * (2 * blocks)
            + [pl.BlockSpec((part, features), lambda i, plane: (i, 0))] * blocks,
            out_specs=[whole] * pieces,
            scratch_shapes=[
                pltpu.VMEM((pieces * each, width), jnp.bfloat16),
                pltpu.VMEM((pieces * each, width), jnp.float32),
            ],
        ),
        out_shape=[jax.ShapeDtypeStruct((each, width), jnp.float32)] * (pieces // 2)
        + [jax.ShapeDtypeStruct((each, width), jnp.bfloat16)] * (pieces - pieces // 2),
        compiler_params=pltpu.CompilerParams(
            dimension_semantics=("arbitrary",), vmem_limit_bytes=60 * 1024 * 1024
        ),
        cost_estimate=pl.CostEstimate(
            flops=6 * pieces * each * width * hidden,
            bytes_accessed=6 * width * hidden + 5 * pieces * each * width,
            transcendentals=pieces * each * hidden,
        ),
        name="layer_products",
    )(plane, *rows, *gates, *ups, *downs)
    return results[: pieces // 2], results[pieces // 2 :]


def head_body(*refs, pieces, columns, tile, lines):
    rows = refs[:pieces]
    labels, weight = refs[pieces : pieces + 2]
    stats_out = refs[pieces + 2]
    gathered, turned, peak, total, picked = refs[pieces + 3 :]
    each = rows[0].shape[0]
    step = pl.program_id(0)
    steps = pl.num_programs(0)

    @pl.when(step == 0)
    def _():
        for i in range(pieces):
            gathered[pl.ds(i * each, each), :] = rows[i][...]
        turned[...] = gathered[...].T
        peak[...] = jnp.full(peak.shape, -1e30, jnp.float32)
        total[...] = jnp.zeros(total.shape, jnp.float32)
        picked[...] = jnp.zeros(picked.shape, jnp.float32)

    count = pieces * each
    some = min(count, 256)
    for first in range(0, count, some):
        span = slice(first, first + some)
        logits = jnp.dot(weight[...], turned[:, span], preferred_element_type=jnp.float32)
        place = step * tile + lax.broadcasted_iota(jnp.int32, (tile, some), 0)
        found = jnp.where(place == labels[:, span], logits, 0.0)
        logits = jnp.where(place < columns, logits, -1e30)
        groups = [slice(i * lines, (i + 1) * lines) for i in range(tile // lines)]
        highest = peak[:, span]
        gained = picked[:, span]
        for group in groups:
            highest = jnp.maximum(highest, logits[group])
            gained = gained + found[group]
        sums = total[:, span] * jnp.exp(peak[:, span] - highest)
        for group in groups:
            sums = sums + jnp.exp(logits[group] - highest)
        peak[:, span] = highest
        total[:, span] = sums
        picked[:, span] = gained

    @pl.when(step == steps - 1)
    def _():
        top = jnp.max(peak[...], axis=0, keepdims=True)
        stats_out[0:1, :] = top
        stats_out[1:2, :] = jnp.sum(total[...] * jnp.exp(peak[...] - top), axis=0, keepdims=True)
        stats_out[2:3, :] = jnp.sum(picked[...], axis=0, keepdims=True)


def head_stats(rows, labels, weight):
    pieces = len(rows)
    each, width = rows[0].shape
    columns = weight.shape[0]
    tile, lines = 512, 8
    count = pieces * each
    whole = pl.BlockSpec((each, width), lambda i: (0, 0))
    return pl.pallas_call(
        lambda *refs: head_body(*refs, pieces=pieces, columns=columns, tile=tile, lines=lines),
        grid=(pl.cdiv(columns, tile),),
        in_specs=[whole] * pieces
        + [
            pl.BlockSpec((1, count), lambda i: (0, 0)),
            pl.BlockSpec((tile, width), lambda i: (i, 0)),
        ],
        out_specs=pl.BlockSpec((3, count), lambda i: (0, 0)),
        out_shape=jax.ShapeDtypeStruct((3, count), jnp.float32),
        scratch_shapes=[
            pltpu.VMEM((count, width), jnp.bfloat16),
            pltpu.VMEM((width, count), jnp.bfloat16),
        ]
        + [pltpu.VMEM((lines, count), jnp.float32)] * 3,
        compiler_params=pltpu.CompilerParams(
            dimension_semantics=("arbitrary",), vmem_limit_bytes=60 * 1024 * 1024
        ),
        cost_estimate=pl.CostEstimate(
            flops=2 * count * width * columns,
            bytes_accessed=2 * width * columns + 2 * count * width,
            transcendentals=count * columns,
        ),
        name="head_stats",
    )(*rows, labels, weight)


def by_planes(*args):
    return planes_step(*args)


def planes_step(entering, depths, targets, norm_gain, w_gate, w_up, w_down, final_gain, head_weight):
    sections = lax.axis_size("section")
    cores = lax.axis_size("vocab")
    my_column = lax.axis_index("section")
    my_core = lax.axis_index("vocab")
    my_plane = lax.axis_index("dp")
    micro_count, _, rows_each, width = entering.shape
    layers = sections
    first_plane = sections // 2 - 1
    plane_of = [(first_plane + layer) % sections for layer in range(layers)]
    my_layer = (my_plane - first_plane) % sections

    def linear(section, core, plane):
        return (section * cores + core) * sections + plane

    micro_ids = jnp.arange(micro_count, dtype=jnp.int32)
    deeper = (depths[None, :] > depths[:, None]) | (
        (depths[None, :] == depths[:, None]) & (micro_ids[None, :] < micro_ids[:, None])
    )
    rank = jnp.sum(deeper.astype(jnp.int32), axis=1)
    hot = rank[None, :] == micro_ids[:, None]
    order = jnp.sum(jnp.where(hot, micro_ids[None, :], 0), axis=1)
    sorted_depths = jnp.sum(jnp.where(hot, depths[None, :], 0), axis=1)
    active_counts = [jnp.sum((depths > layer).astype(jnp.int32)) for layer in range(layers + 1)]

    hidden_each = w_gate.shape[2] // sections

    def column_block(matrix, column):
        if matrix is w_down:
            return lax.dynamic_slice_in_dim(matrix[0], column * hidden_each, hidden_each, 0)
        return lax.dynamic_slice_in_dim(matrix[0], column * hidden_each, hidden_each, 1)

    def across(matrix):
        return [
            swapped(column_block(matrix, my_column ^ mask), "section", mask)
            if mask
            else column_block(matrix, my_column)
            for mask in range(sections)
        ]

    def layer_at(plane):
        return (plane - first_plane) % sections

    early_planes = plane_of[:2]
    late_planes = plane_of[2:]

    def blocks_for(held):
        return [chosen(held, layer_at(my_plane ^ mask) ^ my_column) for mask in range(sections)]

    def towards(blocks, planes, *earlier):
        return [
            swapped(after(blocks[mask], *earlier), "dp", mask, planes) if mask else blocks[0]
            for mask in range(sections)
        ]

    gates = across(w_gate)
    ups = across(w_up)
    downs = across(w_down)
    gates = blocks_for(gates)
    gates_early = towards(gates, early_planes)
    ups = blocks_for(ups)
    ups_early = towards(ups, early_planes)
    downs = blocks_for(downs)
    downs_early = towards(downs, early_planes)
    gates_late = towards(gates, late_planes, *downs_early[1:])
    early = (gates_early, ups_early, downs_early)

    gains = [norm_gain] + [swapped(norm_gain, "section", mask) for mask in range(1, sections)]
    my_gain = chosen(gains, my_layer ^ my_column)
    labels_by = [targets[:, 0]] + [
        swapped(targets[:, 0], "dp", mask) for mask in range(1, sections)
    ]
    labels_all = absolute(jnp.stack(labels_by), my_plane, 0, sections)

    def spread_rows(rows):
        own = [rows] + [swapped(rows, "section", mask) for mask in range(1, sections)]
        return own + [swapped(piece, "vocab", 1) for piece in own]

    def collected(kept, sent):
        total = None
        for mask in reversed(range(sections)):
            both = kept[mask] + swapped(sent[mask], "vocab", 1).astype(jnp.float32)
            if mask:
                both = swapped(both.astype(jnp.bfloat16), "section", mask).astype(jnp.float32)
            total = both if total is None else total + both
        return total

    def run_layer(layer, state, weights, count):
        current = state[:count].reshape(count * rows_each, width)
        rows = spread_rows(rms_scaled(current, my_gain).astype(jnp.bfloat16))
        branch = collected(*layer_products(rows, weights, my_plane[None]))
        moved = (current.astype(jnp.float32) + branch).astype(jnp.bfloat16)
        keep = (sorted_depths[:count] > layer)[:, None, None]
        moved = jnp.where(keep, moved.reshape(count, rows_each, width), state[:count])
        if count < micro_count:
            moved = jnp.concatenate([moved, state[count:]], 0)
        return moved

    def handed_on(state, layer, count):
        pairs = [
            (linear(s, c, plane_of[layer - 1]), linear(s, c, plane_of[layer]))
            for s in range(sections)
            for c in range(cores)
        ]
        arrived = lax.ppermute(state[:count], MESH_AXES, pairs)
        if count < micro_count:
            arrived = jnp.concatenate([arrived, state[count:]], 0)
        return jnp.where(my_plane == plane_of[layer], arrived, state)

    sorted_rows = jnp.concatenate(
        [lax.dynamic_slice_in_dim(entering[:, 0], order[i], 1, 0) for i in range(micro_count)], 0
    )
    pairs = [
        (linear(s, c, s), linear(s, c, plane_of[0])) for s in range(sections) for c in range(cores)
    ]
    state = lax.ppermute(after(sorted_rows, labels_all), MESH_AXES, pairs)
    state = run_layer(0, state, early, micro_count)
    state = handed_on(state, 1, micro_count)
    word = state[0, :8, :128].astype(jnp.float32)
    pairs = [
        (linear(s, c, source), linear(s, c, source ^ 1))
        for s in range(sections)
        for c in range(cores)
        for source in early_planes
    ]
    word = lax.ppermute(word, MESH_AXES, pairs)
    ups_late = towards(ups, late_planes, state, word)
    downs_late = towards(downs, late_planes, state, word)
    late_blocks = (gates_late, ups_late, downs_late)
    sizes = [n for n in range(2, micro_count + 1, 2)]
    for layer in range(1, layers):
        if layer == 2:
            state, late_blocks = lax.optimization_barrier((state, late_blocks))
        weights = early if layer < 2 else late_blocks

        def branch_of(count, layer=layer):
            def run(state, weights):
                if layer > 1:
                    state = handed_on(state, layer, count)
                return run_layer(layer, state, weights, count)

            return run

        which = jnp.clip((active_counts[layer] + 1) // 2 - 1, 0, len(sizes) - 1)
        state = lax.switch(which, [branch_of(n) for n in sizes], state, weights)

    exits_from = chosen(active_counts[1:], my_layer)
    exits_to = chosen(active_counts[:layers], my_layer)
    exit_count = exits_to - exits_from
    most = active_counts[0] - active_counts[1]
    for layer in range(1, layers):
        most = jnp.maximum(most, active_counts[layer] - active_counts[layer + 1])
    column_count = head_weight.shape[1]
    first_column = (my_column * cores + my_core) * column_count
    labels_sorted = jnp.concatenate(
        [lax.dynamic_slice_in_dim(labels_all, order[i], 1, 1) for i in range(micro_count)], 1
    )

    def head(count):
        def run(state, head_columns):
            def window(array, axis):
                padding = [(0, 0)] * array.ndim
                padding[axis] = (0, micro_count)
                return lax.dynamic_slice_in_dim(jnp.pad(array, padding), exits_from, count, axis)

            leaving = window(state, 0).reshape(count * rows_each, width)
            finals = rms_scaled(leaving, final_gain).astype(jnp.bfloat16)
            rows = spread_rows(finals)
            labels = window(labels_sorted, 1).reshape(sections, count, cores, rows_each)
            labels = labels.transpose(2, 0, 1, 3)
            labels = absolute(absolute(labels, my_core, 0, cores), my_column, 1, sections)
            labels = labels.reshape(1, -1) - first_column
            labels = jnp.where(labels < column_count, labels, -1)
            stats = head_stats(rows, labels, head_columns).reshape(3, cores, sections, -1)
            stats = absolute(absolute(stats, my_core, 1, cores), my_column, 2, sections)
            every = lax.all_gather(stats, ("section", "vocab"))
            joined = (every[0, 0], every[0, 1], every[0, 2])
            for i in range(1, sections * cores):
                joined = combine_rows(joined, (every[i, 0], every[i, 1], every[i, 2]))
            losses = jnp.log(joined[1]) + joined[0] - joined[2]
            losses = losses.reshape(cores, sections, count, rows_each).transpose(2, 1, 0, 3)
            losses = losses.reshape(count, sections, cores * rows_each)
            inside = jnp.arange(count) < exit_count
            losses = jnp.where(inside[:, None, None], losses, 0.0)
            table = jnp.zeros((2 * micro_count,) + losses.shape[1:], jnp.float32)
            table = lax.dynamic_update_slice_in_dim(table, losses, exits_from, 0)[:micro_count]
            return table

        return run

    which = jnp.clip((most + 1) // 2 - 1, 0, len(sizes) - 1)
    table = lax.switch(which, [head(n) for n in sizes], state, head_weight.T)
    for mask in (1, 2):
        table = table + swapped(table, "dp", mask)
    mean_loss = jnp.sum(table) / float(table.size)
    token_loss = jnp.sum(jnp.where(hot[:, :, None, None], table[:, None], 0.0), axis=0)
    token_loss = lax.dynamic_slice_in_dim(token_loss, my_plane, 1, 1)
    return (token_loss, mean_loss)


def passed_along(block, axis, distance):
    devices = range(lax.axis_size(axis))
    route = [(i - distance, i) for i in devices if i - distance in devices]
    return lax.ppermute(block, axis, route)


def spread(value, axis, source):
    kept = jnp.where(lax.axis_index(axis) == source, value, 0).astype(value.dtype)
    return lax.psum(kept, axis)


def joined(part, axis, combine):
    gathered = jax.tree.map(lambda a: lax.all_gather(a, axis), part)

    def take(source):
        return jax.tree.map(lambda a: lax.dynamic_index_in_dim(a, source, 0, False), gathered)

    return lax.fori_loop(
        1, lax.axis_size(axis), lambda source, state: combine(state, take(source)), take(0)
    )


def by_sections(entering, depths, targets, norm_gain, w_gate, w_up, w_down, final_gain, head_weight):
    segment_count = lax.axis_size("section")
    my_segment = lax.axis_index("section")
    micro_count = entering.shape[0]
    row_count = entering.shape[2]
    width = entering.shape[3]
    per_segment = w_gate.shape[0]
    gate_full, up_full, down_full = (
        lax.all_gather(w_gate, "dp", axis=1, tiled=True),
        lax.all_gather(w_up, "dp", axis=1, tiled=True),
        lax.all_gather(w_down, "dp", axis=2, tiled=True),
    )
    local_rows = entering[:, 0]

    def apply_layer(layer_index, current):
        normed = rms_scaled(current, norm_gain[layer_index]).astype(jnp.bfloat16)
        block_rows = lax.all_gather(normed, "vocab", axis=0, tiled=True)
        gate_part = jnp.dot(block_rows, gate_full[layer_index], preferred_element_type=jnp.float32)
        up_part = jnp.dot(block_rows, up_full[layer_index], preferred_element_type=jnp.float32)
        hidden = (jax.nn.silu(gate_part) * up_part).astype(jnp.bfloat16)
        branch = lax.psum_scatter(
            jnp.dot(hidden, down_full[layer_index], preferred_element_type=jnp.float32),
            "vocab",
            scatter_dimension=0,
            tiled=True,
        )
        return (current.astype(jnp.float32) + branch).astype(jnp.bfloat16)

    inject_order = jnp.arange(micro_count, dtype=jnp.int32)

    def advance(step_index, carry):
        current, kept_rows = carry
        slot_index = step_index - my_segment
        is_valid = (slot_index >= 0) & (slot_index < micro_count)
        member = inject_order[jnp.clip(slot_index, 0, micro_count - 1)]
        depth_now = jnp.where(is_valid, depths[member], 0)
        fresh_rows = lax.dynamic_index_in_dim(local_rows, member, 0, keepdims=False)
        current = jnp.where(my_segment == 0, fresh_rows, current)
        updated = apply_layer(0, current)
        current = jnp.where(my_segment * per_segment + 0 < depth_now, updated, current)
        record = is_valid & (my_segment == segment_count - 1)
        record_value = current
        previous = lax.dynamic_index_in_dim(kept_rows, member, 0, keepdims=False)
        kept_rows = lax.dynamic_update_index_in_dim(
            kept_rows, jnp.where(record, record_value, previous), member, 0
        )
        current = passed_along(current, "section", 1)
        return (current, kept_rows)

    start_rows = jnp.zeros((row_count, width), jnp.bfloat16)
    start_kept = jnp.zeros((micro_count, row_count, width), jnp.bfloat16)
    _, kept_rows = lax.fori_loop(
        0, micro_count + segment_count - 1, advance, (start_rows, start_kept)
    )
    finals = rms_scaled(kept_rows, final_gain).astype(jnp.bfloat16)
    finals = spread(finals, "section", segment_count - 1)
    share_rows = lax.all_gather(finals, "vocab", axis=1, tiled=True)
    labels = targets[:, 0]
    column_count = head_weight.shape[1]
    first_column = (my_segment * lax.axis_size("vocab") + lax.axis_index("vocab")) * column_count
    logits = jnp.einsum("mpd,dc->mpc", share_rows, head_weight, preferred_element_type=jnp.float32)
    columns = first_column + jnp.arange(column_count, dtype=jnp.int32)
    picked = jnp.sum(jnp.where(columns == labels[:, :, None], logits, 0.0), axis=-1)
    local_peak = jnp.max(logits, axis=-1)
    local_total = jnp.sum(jnp.exp(logits - local_peak[:, :, None]), axis=-1)
    peak_all, totals, target_logit = joined(
        (local_peak, local_total, picked), ("section", "vocab"), combine_rows
    )
    losses = jnp.log(totals) + peak_all - target_logit
    share_sum = lax.psum(jnp.sum(losses), "dp")
    mean_loss = share_sum / float(micro_count * lax.axis_size("dp") * losses.shape[1])
    return (losses[:, None, :], mean_loss)


def solution(mesh):
    in_specs = (
        P(None, "dp", "vocab", None),
        P(),
        P(None, "dp", None),
        P("section", None),
        P("section", "dp", "vocab"),
        P("section", "dp", "vocab"),
        P("section", "vocab", "dp"),
        P(),
        P(None, ("section", "vocab")),
    )
    out_specs = (P(None, "dp", None), P())
    square = mesh.shape["section"] == mesh.shape["dp"] == 4 and mesh.shape["vocab"] == 2
    return jax.shard_map(
        by_planes if square else by_sections,
        mesh=mesh,
        in_specs=in_specs,
        out_specs=out_specs,
        check_vma=False,
    )
```

```python
import jax
import jax.numpy as jnp
from jax import lax
from jax.experimental import pallas as pl
from jax.experimental.pallas import tpu as pltpu
from jax.sharding import PartitionSpec as P


EPS = 1e-05
MESH_AXES = ("section", "vocab", "dp")


def rms_scaled(values, gain):
    widened = values.astype(jnp.float32)
    return widened * lax.rsqrt(jnp.mean(widened * widened, axis=-1, keepdims=True) + EPS) * gain


def combine_rows(first_stats, second_stats):
    peak_one, total_one, picked_one = first_stats
    peak_two, total_two, picked_two = second_stats
    peak_new = jnp.maximum(peak_one, peak_two)
    total_new = total_one * jnp.exp(peak_one - peak_new) + total_two * jnp.exp(peak_two - peak_new)
    return (peak_new, total_new, picked_one + picked_two)


def swapped(block, axis, mask, targets=None):
    size = lax.axis_size(axis)
    pairs = [(i, i ^ mask) for i in range(size) if targets is None or (i ^ mask) in targets]
    return lax.ppermute(block, axis, pairs)


def chosen(options, index):
    result = options[0]
    for k in range(1, len(options)):
        result = jnp.where(index == k, options[k], result)
    return result


def absolute(values, index, axis, size):
    bit = 1
    while bit < size:
        flipped = jnp.concatenate(
            [lax.index_in_dim(values, i ^ bit, axis, True) for i in range(size)], axis
        )
        values = jnp.where((index & bit) != 0, flipped, values)
        bit *= 2
    return values


def after(value, *others):
    return lax.optimization_barrier((value,) + others)[0]


def layer_body(plane, *refs, pieces, blocks, steps, turned):
    rows, refs = refs[:pieces], refs[pieces:]
    gates, ups, downs = refs[:blocks], refs[blocks : 2 * blocks], refs[2 * blocks : 3 * blocks]
    refs = refs[3 * blocks :]
    kept, sent = refs[: pieces // 2], refs[pieces // 2 : pieces]
    gathered, total = refs[pieces:]
    each = rows[0].shape[0]
    features = downs[0].shape[1]
    step = pl.program_id(0)

    def place(mask):
        return pl.ds(pl.multiple_of((plane[0] ^ mask) * features, features), features)

    @pl.when(step == 0)
    def _():
        for i in range(pieces):
            for mask in range(blocks):
                gathered[pl.ds(i * each, each), mask * features : (mask + 1) * features] = rows[i][
                    :, place(mask)
                ]

    count = pieces * each
    tile = min(count, 256)

    def tile_products(index, carry):
        first = pl.multiple_of(index * tile, tile)

        def product(matrices):
            result = None
            for mask in range(blocks):
                here = gathered[pl.ds(first, tile), mask * features : (mask + 1) * features]
                part = lax.dot_general(
                    here,
                    matrices[mask][...],
                    (((1,), (1 if turned else 0,)), ((), ())),
                    preferred_element_type=jnp.float32,
                )
                result = part if result is None else result + part
            return result

        gate_part = product(gates)
        up_part = product(ups)
        hidden = (gate_part / (1.0 + jnp.exp(-gate_part)) * up_part).astype(jnp.bfloat16)
        for mask in range(blocks):
            part = jnp.dot(hidden, downs[mask][...], preferred_element_type=jnp.float32)
            columns = slice(mask * features, (mask + 1) * features)

            @pl.when(step == 0)
            def _(part=part, columns=columns):
                total[pl.ds(first, tile), columns] = part

            @pl.when(step > 0)
            def _(part=part, columns=columns):
                total[pl.ds(first, tile), columns] += part

        return carry

    lax.fori_loop(0, count // tile, tile_products, 0)

    @pl.when(step == steps - 1)
    def _():
        for i in range(pieces):
            for mask in range(blocks):
                block = total[pl.ds(i * each, each), mask * features : (mask + 1) * features]
                if i < pieces // 2:
                    kept[i][:, place(mask)] = block
                else:
                    sent[i - pieces // 2][:, place(mask)] = block.astype(jnp.bfloat16)


def layer_products(rows, weights, plane, part_of=None):
    gates, ups, downs = weights
    pieces, blocks = len(rows), len(gates)
    each, width = rows[0].shape
    hidden, features = downs[0].shape
    turned = part_of is not None
    steps = 2 if hidden % 256 == 0 and not turned else 1
    part = hidden // steps
    if turned:
        across_hidden = pl.BlockSpec((hidden, features), lambda i, plane: (0, part_of))
    else:
        across_hidden = pl.BlockSpec((features, part), lambda i, plane: (0, i))
    whole = pl.BlockSpec((each, width), lambda i, plane: (0, 0))
    results = pl.pallas_call(
        lambda *refs: layer_body(
            *refs, pieces=pieces, blocks=blocks, steps=steps, turned=turned
        ),
        grid_spec=pltpu.PrefetchScalarGridSpec(
            num_scalar_prefetch=1,
            grid=(steps,),
            in_specs=[whole] * pieces
            + [across_hidden] * (2 * blocks)
            + [pl.BlockSpec((part, features), lambda i, plane: (i, 0))] * blocks,
            out_specs=[whole] * pieces,
            scratch_shapes=[
                pltpu.VMEM((pieces * each, width), jnp.bfloat16),
                pltpu.VMEM((pieces * each, width), jnp.float32),
            ],
        ),
        out_shape=[jax.ShapeDtypeStruct((each, width), jnp.float32)] * (pieces // 2)
        + [jax.ShapeDtypeStruct((each, width), jnp.bfloat16)] * (pieces - pieces // 2),
        compiler_params=pltpu.CompilerParams(
            dimension_semantics=("arbitrary",), vmem_limit_bytes=60 * 1024 * 1024
        ),
        cost_estimate=pl.CostEstimate(
            flops=6 * pieces * each * width * hidden,
            bytes_accessed=6 * width * hidden + 5 * pieces * each * width,
            transcendentals=pieces * each * hidden,
        ),
        name="layer_products",
    )(plane, *rows, *gates, *ups, *downs)
    return results[: pieces // 2], results[pieces // 2 :]


def head_body(*refs, pieces, columns, tile, portion, lines):
    rows = refs[:pieces]
    labels, weight = refs[pieces : pieces + 2]
    stats_out = refs[pieces + 2]
    gathered, turned, peak, total, picked = refs[pieces + 3 :]
    each = rows[0].shape[0]
    step = pl.program_id(0)
    steps = pl.num_programs(0)

    @pl.when(step == 0)
    def _():
        for i in range(pieces):
            gathered[pl.ds(i * each, each), :] = rows[i][...]
        turned[...] = gathered[...].T
        peak[...] = jnp.full(peak.shape, -1e30, jnp.float32)
        total[...] = jnp.zeros(total.shape, jnp.float32)
        picked[...] = jnp.zeros(picked.shape, jnp.float32)

    count = pieces * each
    some = min(count, 256)
    for first in range(0, count, some):
        span = slice(first, first + some)
        for part in range(0, tile, portion):
            logits = jnp.dot(
                weight[part : part + portion, :], turned[:, span], preferred_element_type=jnp.float32
            )
            place = step * tile + part + lax.broadcasted_iota(jnp.int32, (portion, some), 0)
            found = jnp.where(place == labels[:, span], logits, 0.0)
            logits = jnp.where(place < columns, logits, -1e30)
            grouped = logits.reshape(portion // lines, lines, some)
            before = peak[:, span]
            highest = jnp.maximum(before, jnp.max(grouped, axis=0))
            sums = jnp.sum(jnp.exp(grouped - highest[None]), axis=0)
            peak[:, span] = highest
            total[:, span] = total[:, span] * jnp.exp(before - highest) + sums
            picked[:, span] += jnp.sum(found.reshape(portion // lines, lines, some), axis=0)

    @pl.when(step == steps - 1)
    def _():
        top = jnp.max(peak[...], axis=0, keepdims=True)
        stats_out[0:1, :] = top
        stats_out[1:2, :] = jnp.sum(total[...] * jnp.exp(peak[...] - top), axis=0, keepdims=True)
        stats_out[2:3, :] = jnp.sum(picked[...], axis=0, keepdims=True)


def head_stats(rows, labels, weight):
    pieces = len(rows)
    each, width = rows[0].shape
    columns = weight.shape[0]
    tile, portion, lines = 1024, 256, 8
    count = pieces * each
    whole = pl.BlockSpec((each, width), lambda i: (0, 0))
    return pl.pallas_call(
        lambda *refs: head_body(
            *refs, pieces=pieces, columns=columns, tile=tile, portion=portion, lines=lines
        ),
        grid=(pl.cdiv(columns, tile),),
        in_specs=[whole] * pieces
        + [
            pl.BlockSpec((1, count), lambda i: (0, 0)),
            pl.BlockSpec((tile, width), lambda i: (i, 0)),
        ],
        out_specs=pl.BlockSpec((3, count), lambda i: (0, 0)),
        out_shape=jax.ShapeDtypeStruct((3, count), jnp.float32),
        scratch_shapes=[
            pltpu.VMEM((count, width), jnp.bfloat16),
            pltpu.VMEM((width, count), jnp.bfloat16),
        ]
        + [pltpu.VMEM((lines, count), jnp.float32)] * 3,
        compiler_params=pltpu.CompilerParams(
            dimension_semantics=("arbitrary",), vmem_limit_bytes=60 * 1024 * 1024
        ),
        cost_estimate=pl.CostEstimate(
            flops=2 * count * width * columns,
            bytes_accessed=2 * width * columns + 2 * count * width,
            transcendentals=count * columns,
        ),
        name="head_stats",
    )(*rows, labels, weight)


def by_planes(*args):
    return planes_step(*args)


def planes_step(entering, depths, targets, norm_gain, w_gate, w_up, w_down, final_gain, head_weight):
    sections = lax.axis_size("section")
    cores = lax.axis_size("vocab")
    my_column = lax.axis_index("section")
    my_core = lax.axis_index("vocab")
    my_plane = lax.axis_index("dp")
    micro_count, _, rows_each, width = entering.shape
    layers = sections
    first_plane = sections // 2 - 1
    plane_of = [(first_plane + layer) % sections for layer in range(layers)]
    my_layer = (my_plane - first_plane) % sections

    def linear(section, core, plane):
        return (section * cores + core) * sections + plane

    micro_ids = jnp.arange(micro_count, dtype=jnp.int32)
    deeper = (depths[None, :] > depths[:, None]) | (
        (depths[None, :] == depths[:, None]) & (micro_ids[None, :] < micro_ids[:, None])
    )
    rank = jnp.sum(deeper.astype(jnp.int32), axis=1)
    hot = rank[None, :] == micro_ids[:, None]
    order = jnp.sum(jnp.where(hot, micro_ids[None, :], 0), axis=1)
    sorted_depths = jnp.sum(jnp.where(hot, depths[None, :], 0), axis=1)
    active_counts = [jnp.sum((depths > layer).astype(jnp.int32)) for layer in range(layers + 1)]

    hidden_each = w_gate.shape[2] // sections

    def column_block(matrix, column):
        if matrix is w_down:
            return lax.dynamic_slice_in_dim(matrix[0], column * hidden_each, hidden_each, 0)
        return lax.dynamic_slice_in_dim(matrix[0], column * hidden_each, hidden_each, 1)

    def across(matrix, *earlier):
        return [
            swapped(after(column_block(matrix, my_column ^ mask), *earlier), "section", mask)
            if mask
            else column_block(matrix, my_column)
            for mask in range(sections)
        ]

    def layer_at(plane):
        return (plane - first_plane) % sections

    early_planes = plane_of[:2]
    late_planes = plane_of[2:]

    def blocks_for(held):
        return [chosen(held, layer_at(my_plane ^ mask) ^ my_column) for mask in range(sections)]

    def halves_for(held, layer, axis):
        block = chosen(held, layer ^ my_column)
        first, second = jnp.split(block, 2, axis)
        return [
            jnp.where((my_plane ^ mask) == early_planes[0], first, second)
            for mask in range(sections)
        ]

    def towards(blocks, planes, *earlier):
        return [
            swapped(after(blocks[mask], *earlier), "dp", mask, planes) if mask else blocks[0]
            for mask in range(sections)
        ]

    def both_halves(held, axis):
        return [halves_for(held, layer, axis) for layer in range(2)]

    def stacked(halves):
        return [jnp.concatenate(pair, 0) for pair in zip(*halves)]

    gains = [norm_gain] + [swapped(norm_gain, "section", mask) for mask in range(1, sections)]

    def gain_of(layer, *earlier):
        held = lax.optimization_barrier((tuple(gains), earlier))[0]
        return chosen(held, layer ^ my_column)

    gates = across(w_gate)
    gate_halves = stacked(both_halves(gates, 1))
    ups = across(w_up, *gates[1:])
    gates_early = towards(gate_halves, early_planes)
    gain_first = gain_of(0, *gate_halves)
    ups = lax.optimization_barrier((ups, gate_halves))[0]
    up_halves = stacked(both_halves(ups, 1))
    downs = across(w_down, *ups[1:])
    ups_early = towards(up_halves, early_planes)
    gain_second = gain_of(1, *up_halves)
    downs = lax.optimization_barrier((downs, up_halves))[0]
    downs_early = []
    for halves in both_halves(downs, 0):
        downs_early.append(towards(halves, early_planes))
    gates, ups, downs = blocks_for(gates), blocks_for(ups), blocks_for(downs)
    gates_late = towards(gates, late_planes, *downs_early[0][1:])
    gates_early, ups_early = [block.T for block in gates_early], [block.T for block in ups_early]
    early = [(gates_early, ups_early, downs_early[layer]) for layer in range(2)]

    layer_gains = [gain_first, gain_second]
    layer_gains += [chosen(gains, my_layer ^ my_column)] * (layers - 2)
    labels_by = [targets[:, 0]] + [
        swapped(targets[:, 0], "dp", mask) for mask in range(1, sections)
    ]
    labels_all = absolute(jnp.stack(labels_by), my_plane, 0, sections)

    def spread_rows(rows):
        own = [rows] + [swapped(rows, "section", mask) for mask in range(1, sections)]
        return own + [swapped(piece, "vocab", 1) for piece in own]

    def collected(kept, sent):
        total = None
        for mask in reversed(range(sections)):
            both = kept[mask] + swapped(sent[mask], "vocab", 1).astype(jnp.float32)
            if mask:
                both = swapped(both.astype(jnp.bfloat16), "section", mask).astype(jnp.float32)
            total = both if total is None else total + both
        return total

    def run_layer(layer, state, weights, count):
        current = state[:count].reshape(count * rows_each, width)
        rows = spread_rows(rms_scaled(current, layer_gains[layer]).astype(jnp.bfloat16))
        branch = collected(*layer_products(rows, weights, my_plane[None], layer if layer < 2 else 0))
        if layer < 2:
            mine = branch.astype(jnp.bfloat16)
            other = swapped(mine, "dp", early_planes[0] ^ early_planes[1], early_planes)
            branch = mine.astype(jnp.float32) + other.astype(jnp.float32)
        moved = (current.astype(jnp.float32) + branch).astype(jnp.bfloat16)
        keep = (sorted_depths[:count] > layer)[:, None, None]
        moved = jnp.where(keep, moved.reshape(count, rows_each, width), state[:count])
        if count < micro_count:
            moved = jnp.concatenate([moved, state[count:]], 0)
        return moved

    def handed_on(state, layer, count):
        pairs = [
            (linear(s, c, plane_of[layer - 1]), linear(s, c, plane_of[layer]))
            for s in range(sections)
            for c in range(cores)
        ]
        arrived = lax.ppermute(state[:count], MESH_AXES, pairs)
        if count < micro_count:
            arrived = jnp.concatenate([arrived, state[count:]], 0)
        return jnp.where(my_plane == plane_of[layer], arrived, state)

    sorted_rows = jnp.concatenate(
        [lax.dynamic_slice_in_dim(entering[:, 0], order[i], 1, 0) for i in range(micro_count)], 0
    )
    sorted_rows = after(sorted_rows, labels_all)
    arrivals = [
        lax.ppermute(
            sorted_rows,
            MESH_AXES,
            [(linear(s, c, s), linear(s, c, plane)) for s in range(sections) for c in range(cores)],
        )
        for plane in early_planes
    ]
    state = jnp.where(my_plane == early_planes[0], arrivals[0], arrivals[1])
    state = run_layer(0, state, early[0], micro_count)
    word = state[0, :8, :128].astype(jnp.float32)
    pairs = [
        (linear(s, c, source), linear(s, c, source ^ 1))
        for s in range(sections)
        for c in range(cores)
        for source in early_planes
    ]
    word = lax.ppermute(word, MESH_AXES, pairs)
    ups_late = towards(ups, late_planes, state, word)
    downs_late = towards(downs, late_planes, state, word)
    late_blocks = ([b.T for b in gates_late], [b.T for b in ups_late], downs_late)
    sizes = [n for n in range(2, micro_count + 1, 2)]
    for layer in range(1, layers):
        if layer == 2:
            state, late_blocks = lax.optimization_barrier((state, late_blocks))
        weights = early[1] if layer < 2 else late_blocks

        def branch_of(count, layer=layer):
            def run(state, weights):
                if layer > 1:
                    state = handed_on(state, layer, count)
                return run_layer(layer, state, weights, count)

            return run

        which = jnp.clip((active_counts[layer] + 1) // 2 - 1, 0, len(sizes) - 1)
        state = lax.switch(which, [branch_of(n) for n in sizes], state, weights)

    exits_from = chosen(active_counts[1:], my_layer)
    exits_to = chosen(active_counts[:layers], my_layer)
    exit_count = exits_to - exits_from
    most = active_counts[0] - active_counts[1]
    for layer in range(1, layers):
        most = jnp.maximum(most, active_counts[layer] - active_counts[layer + 1])
    column_count = head_weight.shape[1]
    first_column = (my_column * cores + my_core) * column_count
    labels_sorted = jnp.concatenate(
        [lax.dynamic_slice_in_dim(labels_all, order[i], 1, 1) for i in range(micro_count)], 1
    )

    def head(count):
        def run(state, head_columns):
            def window(array, axis):
                padding = [(0, 0)] * array.ndim
                padding[axis] = (0, micro_count)
                return lax.dynamic_slice_in_dim(jnp.pad(array, padding), exits_from, count, axis)

            leaving = window(state, 0).reshape(count * rows_each, width)
            finals = rms_scaled(leaving, final_gain).astype(jnp.bfloat16)
            rows = spread_rows(finals)
            labels = window(labels_sorted, 1).reshape(sections, count, cores, rows_each)
            labels = labels.transpose(2, 0, 1, 3)
            labels = absolute(absolute(labels, my_core, 0, cores), my_column, 1, sections)
            labels = labels.reshape(1, -1) - first_column
            labels = jnp.where(labels < column_count, labels, -1)
            stats = head_stats(rows, labels, head_columns).reshape(3, cores, sections, -1)
            stats = absolute(absolute(stats, my_core, 1, cores), my_column, 2, sections)
            every = lax.all_gather(stats, ("section", "vocab"))
            joined = (every[0, 0], every[0, 1], every[0, 2])
            for i in range(1, sections * cores):
                joined = combine_rows(joined, (every[i, 0], every[i, 1], every[i, 2]))
            losses = jnp.log(joined[1]) + joined[0] - joined[2]
            losses = losses.reshape(cores, sections, count, rows_each).transpose(2, 1, 0, 3)
            losses = losses.reshape(count, sections, cores * rows_each)
            inside = jnp.arange(count) < exit_count
            losses = jnp.where(inside[:, None, None], losses, 0.0)
            table = jnp.zeros((2 * micro_count,) + losses.shape[1:], jnp.float32)
            table = lax.dynamic_update_slice_in_dim(table, losses, exits_from, 0)[:micro_count]
            return table

        return run

    which = jnp.clip((most + 1) // 2 - 1, 0, len(sizes) - 1)
    table = lax.switch(which, [head(n) for n in sizes], state, head_weight.T)
    for mask in (1, 2):
        table = table + swapped(table, "dp", mask)
    mean_loss = jnp.sum(table) / float(table.size)
    token_loss = jnp.sum(jnp.where(hot[:, :, None, None], table[:, None], 0.0), axis=0)
    token_loss = lax.dynamic_slice_in_dim(token_loss, my_plane, 1, 1)
    return (token_loss, mean_loss)


def passed_along(block, axis, distance):
    devices = range(lax.axis_size(axis))
    route = [(i - distance, i) for i in devices if i - distance in devices]
    return lax.ppermute(block, axis, route)


def spread(value, axis, source):
    kept = jnp.where(lax.axis_index(axis) == source, value, 0).astype(value.dtype)
    return lax.psum(kept, axis)


def joined(part, axis, combine):
    gathered = jax.tree.map(lambda a: lax.all_gather(a, axis), part)

    def take(source):
        return jax.tree.map(lambda a: lax.dynamic_index_in_dim(a, source, 0, False), gathered)

    return lax.fori_loop(
        1, lax.axis_size(axis), lambda source, state: combine(state, take(source)), take(0)
    )


def by_sections(entering, depths, targets, norm_gain, w_gate, w_up, w_down, final_gain, head_weight):
    segment_count = lax.axis_size("section")
    my_segment = lax.axis_index("section")
    micro_count = entering.shape[0]
    row_count = entering.shape[2]
    width = entering.shape[3]
    per_segment = w_gate.shape[0]
    gate_full, up_full, down_full = (
        lax.all_gather(w_gate, "dp", axis=1, tiled=True),
        lax.all_gather(w_up, "dp", axis=1, tiled=True),
        lax.all_gather(w_down, "dp", axis=2, tiled=True),
    )
    local_rows = entering[:, 0]

    def apply_layer(layer_index, current):
        normed = rms_scaled(current, norm_gain[layer_index]).astype(jnp.bfloat16)
        block_rows = lax.all_gather(normed, "vocab", axis=0, tiled=True)
        gate_part = jnp.dot(block_rows, gate_full[layer_index], preferred_element_type=jnp.float32)
        up_part = jnp.dot(block_rows, up_full[layer_index], preferred_element_type=jnp.float32)
        hidden = (jax.nn.silu(gate_part) * up_part).astype(jnp.bfloat16)
        branch = lax.psum_scatter(
            jnp.dot(hidden, down_full[layer_index], preferred_element_type=jnp.float32),
            "vocab",
            scatter_dimension=0,
            tiled=True,
        )
        return (current.astype(jnp.float32) + branch).astype(jnp.bfloat16)

    inject_order = jnp.arange(micro_count, dtype=jnp.int32)

    def advance(step_index, carry):
        current, kept_rows = carry
        slot_index = step_index - my_segment
        is_valid = (slot_index >= 0) & (slot_index < micro_count)
        member = inject_order[jnp.clip(slot_index, 0, micro_count - 1)]
        depth_now = jnp.where(is_valid, depths[member], 0)
        fresh_rows = lax.dynamic_index_in_dim(local_rows, member, 0, keepdims=False)
        current = jnp.where(my_segment == 0, fresh_rows, current)
        updated = apply_layer(0, current)
        current = jnp.where(my_segment * per_segment + 0 < depth_now, updated, current)
        record = is_valid & (my_segment == segment_count - 1)
        record_value = current
        previous = lax.dynamic_index_in_dim(kept_rows, member, 0, keepdims=False)
        kept_rows = lax.dynamic_update_index_in_dim(
            kept_rows, jnp.where(record, record_value, previous), member, 0
        )
        current = passed_along(current, "section", 1)
        return (current, kept_rows)

    start_rows = jnp.zeros((row_count, width), jnp.bfloat16)
    start_kept = jnp.zeros((micro_count, row_count, width), jnp.bfloat16)
    _, kept_rows = lax.fori_loop(
        0, micro_count + segment_count - 1, advance, (start_rows, start_kept)
    )
    finals = rms_scaled(kept_rows, final_gain).astype(jnp.bfloat16)
    finals = spread(finals, "section", segment_count - 1)
    share_rows = lax.all_gather(finals, "vocab", axis=1, tiled=True)
    labels = targets[:, 0]
    column_count = head_weight.shape[1]
    first_column = (my_segment * lax.axis_size("vocab") + lax.axis_index("vocab")) * column_count
    logits = jnp.einsum("mpd,dc->mpc", share_rows, head_weight, preferred_element_type=jnp.float32)
    columns = first_column + jnp.arange(column_count, dtype=jnp.int32)
    picked = jnp.sum(jnp.where(columns == labels[:, :, None], logits, 0.0), axis=-1)
    local_peak = jnp.max(logits, axis=-1)
    local_total = jnp.sum(jnp.exp(logits - local_peak[:, :, None]), axis=-1)
    peak_all, totals, target_logit = joined(
        (local_peak, local_total, picked), ("section", "vocab"), combine_rows
    )
    losses = jnp.log(totals) + peak_all - target_logit
    share_sum = lax.psum(jnp.sum(losses), "dp")
    mean_loss = share_sum / float(micro_count * lax.axis_size("dp") * losses.shape[1])
    return (losses[:, None, :], mean_loss)


def solution(mesh):
    in_specs = (
        P(None, "dp", "vocab", None),
        P(),
        P(None, "dp", None),
        P("section", None),
        P("section", "dp", "vocab"),
        P("section", "dp", "vocab"),
        P("section", "vocab", "dp"),
        P(),
        P(None, ("section", "vocab")),
    )
    out_specs = (P(None, "dp", None), P())
    square = mesh.shape["section"] == mesh.shape["dp"] == 4 and mesh.shape["vocab"] == 2
    return jax.shard_map(
        by_planes if square else by_sections,
        mesh=mesh,
        in_specs=in_specs,
        out_specs=out_specs,
        check_vma=False,
    )
```
